32 devices in a mesh: zero: 8 (over y, x, core), width: 4 (over z).
Axes of the slice: x: 2, y: 2, z: 4, core: 2. Of those that a mesh axis runs over, the one named last changes fastest.
Arguments:
- train_query: bfloat16 [3584, 4096], P('zero', 'width'), may hold values from -0.09375 to 0.09375
- low_query: bfloat16 [3584, 32], P('zero'), may hold values from -0.09375 to 0.09375
- high_query: bfloat16 [32, 4096], P(None, 'width'), may hold values from -1 to 1
- train_key: bfloat16 [3584, 2048], P('zero', 'width'), may hold values from -0.09375 to 0.09375
- low_key: bfloat16 [3584, 32], P('zero'), may hold values from -0.09375 to 0.09375
- high_key: bfloat16 [32, 2048], P(None, 'width'), may hold values from -1 to 1
- train_value: bfloat16 [3584, 2048], P('zero', 'width'), may hold values from -0.09375 to 0.09375
- low_value: bfloat16 [3584, 32], P('zero'), may hold values from -0.09375 to 0.09375
- high_value: bfloat16 [32, 2048], P(None, 'width'), may hold values from -1 to 1
- train_mixed: bfloat16 [4096, 3584], P('width', 'zero'), may hold values from -0.09375 to 0.09375
- low_mixed: bfloat16 [4096, 32], P('width'), may hold values from -0.09375 to 0.09375
- high_mixed: bfloat16 [32, 3584], P(None, 'zero'), may hold values from -1 to 1
- norm_train: float32 [3584], P(('zero', 'width')), may hold values from 0.25 to 1.75
- norm_step: float32 [3584], P(('zero', 'width')), may hold values from -0.3 to 0.3
Outputs:
- ready_query: bfloat16 [4096, 3584], P('width')
- ready_key: bfloat16 [2048, 3584], P('width')
- ready_value: bfloat16 [2048, 3584], P('width')
- ready_mixed: bfloat16 [3584, 4096], P(None, 'width')
- serve_norm: bfloat16 [3584], replicated
The draws below stay inside these ranges and needn't reach their ends.
All inputs are finite; a program needn't handle non-finite values.
Results may differ from the reference program's by a relative error of at most 0.001.
Values may be sent and summed in bfloat16 or wider, within the bound.
A program may use at most 128 MiB of HBM per device.

```python
import jax
import jax.numpy as jnp

D_MODEL = 3584
Q_DIM = 4096
KV_DIM = 2048
RANK = 32


def level_of(rng, extent, cuts, least, high):
    def one(dim, blocks):
        draws = jax.random.uniform(jax.random.fold_in(jax.random.fold_in(rng, 6), dim), (blocks,), jnp.float32, least / len(cuts), high / len(cuts))
        return jnp.repeat(jnp.exp(draws), extent[dim] // blocks).reshape((-1,) + (1,) * (len(extent) - dim - 1))

    gain = one(*cuts[0])
    for cut in cuts[1:]:
        gain = gain * one(*cut)
    return gain


def normal_values(own_key, extent, spread, most, cuts=(), held_as=jnp.bfloat16):
    drawn = jax.random.normal(own_key, extent, jnp.float32) * spread
    if len(cuts) > 0:
        drawn = level_of(own_key, extent, cuts, -0.22, 0.18) * drawn
    return jnp.clip(drawn, min=-most, max=most).astype(held_as)


def setup_inputs(seed: int = 0) -> dict:
    seeds = jax.random.split(jax.random.key(seed), 15)
    return {
        "train_query": normal_values(seeds[0], (D_MODEL, Q_DIM), D_MODEL ** -0.5, 0.09375, ((0, 8), (1, 4))),
        "low_query": normal_values(seeds[1], (D_MODEL, RANK), D_MODEL ** -0.5, 0.09375, ((0, 8),)),
        "high_query": normal_values(seeds[2], (RANK, Q_DIM), RANK ** -0.5, 1.0, ((1, 4),)),
        "train_key": normal_values(seeds[3], (D_MODEL, KV_DIM), D_MODEL ** -0.5, 0.09375, ((0, 8), (1, 4))),
        "low_key": normal_values(seeds[4], (D_MODEL, RANK), D_MODEL ** -0.5, 0.09375, ((0, 8),)),
        "high_key": normal_values(seeds[5], (RANK, KV_DIM), RANK ** -0.5, 1.0, ((1, 4),)),
        "train_value": normal_values(seeds[6], (D_MODEL, KV_DIM), D_MODEL ** -0.5, 0.09375, ((0, 8), (1, 4))),
        "low_value": normal_values(seeds[7], (D_MODEL, RANK), D_MODEL ** -0.5, 0.09375, ((0, 8),)),
        "high_value": normal_values(seeds[8], (RANK, KV_DIM), RANK ** -0.5, 1.0, ((1, 4),)),
        "train_mixed": normal_values(seeds[9], (Q_DIM, D_MODEL), Q_DIM ** -0.5, 0.09375, ((0, 4), (1, 8))),
        "low_mixed": normal_values(seeds[10], (Q_DIM, RANK), Q_DIM ** -0.5, 0.09375, ((0, 4),)),
        "high_mixed": normal_values(seeds[11], (RANK, D_MODEL), RANK ** -0.5, 1.0, ((1, 8),)),
        "norm_train": jnp.clip(1.0 + 0.15 * jax.random.normal(seeds[12], (D_MODEL,), jnp.float32), 0.25, 1.75),
        "norm_step": jnp.clip(jax.random.uniform(seeds[13], (D_MODEL,), jnp.float32, -0.3, 0.3) * level_of(seeds[13], (D_MODEL,), ((0, 32),), -0.4, 0.0), -0.3, 0.3),
    }


mix_rate = 0.5


def reference(train_query, low_query, high_query, train_key, low_key, high_key, train_value, low_value, high_value, train_mixed, low_mixed, high_mixed, norm_train, norm_step):
    latest_query = train_query.astype(jnp.float32) + mix_rate * jnp.dot(low_query, high_query, preferred_element_type=jnp.float32)
    latest_key = train_key.astype(jnp.float32) + mix_rate * jnp.dot(low_key, high_key, preferred_element_type=jnp.float32)
    latest_value = train_value.astype(jnp.float32) + mix_rate * jnp.dot(low_value, high_value, preferred_element_type=jnp.float32)
    latest_mixed = train_mixed.astype(jnp.float32) + mix_rate * jnp.dot(low_mixed, high_mixed, preferred_element_type=jnp.float32)
    ready_query = latest_query.T.astype(jnp.bfloat16)
    ready_key = latest_key.T.astype(jnp.bfloat16)
    ready_value = latest_value.T.astype(jnp.bfloat16)
    ready_mixed = latest_mixed.T.astype(jnp.bfloat16)
    serve_norm = (norm_train + norm_step).astype(jnp.bfloat16)
    return ready_query, ready_key, ready_value, ready_mixed, serve_norm
```

```python
import functools
import math

import jax
import jax.numpy as jnp
from jax import lax
from jax.experimental import pallas as pl
from jax.experimental.pallas import tpu as pltpu
from jax.sharding import PartitionSpec as P

mix_rate = 0.5
CORES = 2
LANES = 128
F32 = jnp.float32
BF16 = jnp.bfloat16


def plain_body(
    train_query, low_query, high_query, train_key, low_key, high_key, train_value, low_value, high_value,
    train_mixed, low_mixed, high_mixed, norm_train, norm_step,
):
    def merged(train, low, high):
        return (train.astype(F32) + mix_rate * jnp.dot(low, high, preferred_element_type=F32)).astype(BF16)

    return (
        lax.all_gather(merged(train_query, low_query, high_query), "zero", axis=0, tiled=True).T,
        lax.all_gather(merged(train_key, low_key, high_key), "zero", axis=0, tiled=True).T,
        lax.all_gather(merged(train_value, low_value, high_value), "zero", axis=0, tiled=True).T,
        lax.all_gather(merged(train_mixed, low_mixed, high_mixed).T, "zero", axis=0, tiled=True),
        lax.all_gather((norm_train + norm_step).astype(BF16), ("zero", "width"), axis=0, tiled=True),
    )


def kernel(
    zeros, widths,
    tq, lq, hq, tk, lk, hk, tv, lv, hv, tm, lm, hm, nt, ns,
    oq, ok, ov, om, norm_out,
    on, own_q, own_k, own_v, own_m, pq, pk, pv, plq, plk, plv, keep, swap_send, swap_recv, send, recv, nsend, nrecv,
):
    me, w = lax.axis_index("zero"), lax.axis_index("width")
    c = lax.rem(me, 2)
    x = lax.rem(lax.div(me, 2), 2)
    y = lax.div(me, 4)
    chip = lax.div(me, 2)
    partner, xn, yn = me + 1 - 2 * c, me + 2 - 4 * x, me + 4 - 8 * y
    chip_x, chip_y, chip_d = chip + 1 - 2 * x, chip + 2 - 4 * y, 3 - chip
    rows = tq.shape[0]
    pair = 2 * rows

    def remote(src, dst, ssem, rsem, **where):
        return pltpu.make_async_remote_copy(
            src_ref=src, dst_ref=dst, send_sem=ssem, recv_sem=rsem,
            device_id=where, device_id_type=pl.DeviceIdType.MESH,
        )

    others = [lax.rem(me + d, zeros) for d in range(1, zeros)]
    barrier = pltpu.get_barrier_semaphore()
    for other in others:
        pl.semaphore_signal(barrier, inc=1, device_id={"zero": other}, device_id_type=pl.DeviceIdType.MESH)
    for d in range(1, widths):
        pl.semaphore_signal(
            barrier, inc=1, device_id={"width": lax.rem(w + d, widths)}, device_id_type=pl.DeviceIdType.MESH
        )
    pl.semaphore_wait(barrier, zeros + widths - 2)

    mine = pl.ds(pl.multiple_of(rows * c, 16), rows)
    swaps = []
    for k, (train, low, held, held_low) in enumerate(((tq, lq, pq, plq), (tk, lk, pk, plk), (tv, lv, pv, plv))):
        half = train.shape[1] // 2
        cols = pl.ds(pl.multiple_of((1 - c) * half, LANES), half)
        for e, (src, dst) in enumerate(((train.at[:, cols], held.at[mine, :]), (low, held_low.at[mine, :]))):
            copy = remote(src, dst, swap_send.at[2 * k + e], swap_recv.at[2 * k + e], zero=partner)
            copy.start()
            swaps.append(copy)

    on[me, w] = jnp.pad(nt[...] + ns[...], ((0, 0), (0, LANES - nt.shape[1])))
    for train, low, held, held_low in ((tq, lq, pq, plq), (tk, lk, pk, plk), (tv, lv, pv, plv)):
        half = train.shape[1] // 2
        held[mine, :] = train[:, pl.ds(pl.multiple_of(c * half, LANES), half)]
        held_low[mine, :] = low[...]
    small = []
    for d in range(1, widths):
        copy = remote(
            on.at[me, w], on.at[me, w], nsend.at[d - 1], nrecv.at[d - 1], width=lax.rem(w + d, widths)
        )
        copy.start()
        small.append(copy)

    for i in range(tm.shape[0] // LANES):
        at = slice(i * LANES, (i + 1) * LANES)
        merged = tm[at, :].astype(F32) + mix_rate * jnp.dot(lm[at, :], hm[...], preferred_element_type=F32)
        own_m[:, at] = merged.T.astype(BF16)
    kept = [pltpu.make_async_copy(own_m, om.at[pl.ds(pl.multiple_of(rows * me, 16), rows), :], keep.at[3])]
    kept[0].start()

    for copy in small:
        copy.wait()
    for d in range(1, zeros):
        copy = remote(
            on.at[me], on.at[me], nsend.at[widths - 2 + d], nrecv.at[widths - 2 + d], zero=others[d - 1]
        )
        copy.start()
        small.append(copy)

    part = rows // 2

    def mixed_item(h):
        return lambda p, cc: om.at[pl.ds(pl.multiple_of(rows * (2 * p + cc) + h * part, 16), part), :]

    def item(out, start, size, share):
        return lambda p, cc: out.at[
            pl.ds(pl.multiple_of(share * cc + start, 16), size), pl.ds(pl.multiple_of(pair * p, LANES), pair)
        ]

    nq, nk = oq.shape[0] // 2, ok.shape[0] // 2
    first = [mixed_item(0), item(oq, 0, nq // 2, nq), item(ok, 0, nk, nk)]
    second = [mixed_item(1), item(oq, nq // 2, nq // 2, nq), item(ov, 0, nk, nk)]
    items = first + second
    sources = [
        own_m.at[:part, :], own_q.at[: nq // 2, :], own_k, own_m.at[part:, :], own_q.at[nq // 2 :, :], own_v
    ]
    n = len(first)
    TO_X, TO_Y, ON, P_OWN, P_X, P_Y, P_D = range(7)
    copies = {}

    def go(k, kind, p, where):
        region = items[k](p, c)
        source = sources[k] if kind in (TO_X, TO_Y, P_OWN) else region
        copy = remote(source, region, send.at[k, kind], recv.at[k, kind], zero=where)
        copy.start()
        copies[k, kind] = copy

    def own(j):
        go(j, TO_X, chip, xn)
        go(n + j, TO_Y, chip, yn)

    own(0)

    def merge(e, out, own_out, held, held_low, high):
        half = held.shape[1]
        cols = pl.ds(pl.multiple_of(c * half, LANES), half)
        for j in range(pair // LANES):
            at = slice(j * LANES, (j + 1) * LANES)
            merged = held[at, :].astype(F32) + mix_rate * jnp.dot(
                held_low[at, :], high[:, cols], preferred_element_type=F32
            )
            own_out[:, at] = merged.T.astype(BF16)
        here = out.at[
            pl.ds(pl.multiple_of(c * half, 16), half), pl.ds(pl.multiple_of(pair * chip, LANES), pair)
        ]
        kept.append(pltpu.make_async_copy(own_out, here, keep.at[e]))
        kept[-1].start()

    for copy in swaps:
        copy.wait()
    merge(0, oq, own_q, pq, plq, hq)
    own(1)
    merge(1, ok, own_k, pk, plk, hk)
    merge(2, ov, own_v, pv, plv, hv)
    own(2)
    for j in range(n):
        go(n + j, TO_X, chip, xn)
        go(j, TO_Y, chip, yn)
    for k in range(2 * n):
        go(k, P_OWN, chip, partner)

    for j in range(n):
        copies[j, TO_X].wait_recv()
        go(j, ON, chip_x, yn)
        go(j, P_X, chip_x, partner)
        copies[n + j, TO_Y].wait_recv()
        go(n + j, ON, chip_y, xn)
        go(n + j, P_Y, chip_y, partner)
    for j in range(n):
        copies[n + j, TO_X].wait_recv()
        go(n + j, P_X, chip_x, partner)
        copies[j, TO_Y].wait_recv()
        go(j, P_Y, chip_y, partner)
    for j in range(n):
        for k in (j, n + j):
            copies[k, ON].wait_recv()
            go(k, P_D, chip_d, partner)
    for copy in kept:
        copy.wait()
    for copy in small[widths - 1 :]:
        copy.wait()
    norm_out[...] = on[...]
    for (k, kind), copy in copies.items():
        copy.wait_send()
        if kind >= P_OWN:
            copy.wait_recv()


def fast_body(zeros, widths, *args):
    tq, lq, hq, tk, lk, hk, tv, lv, hv, tm, lm, hm, nt, ns = args
    depth = tq.shape[0] * zeros
    VM = pltpu.VMEM
    new = jax.ShapeDtypeStruct
    outs = [
        new((tq.shape[1], depth), BF16), new((tk.shape[1], depth), BF16), new((tv.shape[1], depth), BF16),
        new((depth, tm.shape[0]), BF16), new((zeros, widths, 1, LANES), F32),
    ]
    pair = 2 * tq.shape[0]
    dma = pltpu.SemaphoreType.DMA
    small = widths - 1 + zeros - 1
    oq, ok, ov, om, on = pl.pallas_call(
        functools.partial(kernel, zeros, widths),
        out_shape=outs,
        in_specs=[pl.BlockSpec(memory_space=VM)] * len(args),
        out_specs=[pl.BlockSpec(memory_space=m) for m in (pl.ANY,) * 4 + (VM,)],
        scratch_shapes=[
            VM((zeros, widths, 1, LANES), F32),
            VM((tq.shape[1] // 2, pair), BF16), VM((tk.shape[1] // 2, pair), BF16), VM((tv.shape[1] // 2, pair), BF16),
            VM((tm.shape[1], tm.shape[0]), BF16),
            VM((pair, tq.shape[1] // 2), BF16), VM((pair, tk.shape[1] // 2), BF16), VM((pair, tv.shape[1] // 2), BF16),
            VM((pair, lq.shape[1]), BF16), VM((pair, lk.shape[1]), BF16), VM((pair, lv.shape[1]), BF16),
            dma((4,)), dma((6,)), dma((6,)), dma((6, 7)), dma((6, 7)), dma((small,)), dma((small,)),
        ],
        compiler_params=pltpu.CompilerParams(
            collective_id=0, has_side_effects=True, vmem_limit_bytes=30 * 2**20
        ),
        name="gather_merged",
    )(tq, lq, hq, tk, lk, hk, tv, lv, hv, tm, lm, hm, nt[None, :], ns[None, :])
    norm = on[:, :, 0, : nt.shape[0]].reshape(-1).astype(BF16)
    return oq, ok, ov, om, norm


def solution(mesh):
    placed = (
        P("zero", "width"), P("zero", None), P(None, "width"),
        P("zero", "width"), P("zero", None), P(None, "width"),
        P("zero", "width"), P("zero", None), P(None, "width"),
        P("width", "zero"), P("width", None), P(None, "zero"),
        P(("zero", "width")), P(("zero", "width")),
    )
    zeros, widths = mesh.shape["zero"], mesh.shape["width"]
    side = math.isqrt(zeros // CORES)

    def body(*args):
        rows = args[0].shape[0]
        square = side == 2 and CORES * side * side == zeros
        if square and CORES * rows % LANES == 0 and rows % 32 == 0:
            return fast_body(zeros, widths, *args)
        return plain_body(*args)

    return jax.shard_map(
        body,
        mesh=mesh,
        in_specs=placed,
        out_specs=(P("width", None), P("width", None), P("width", None), P(None, "width"), P()),
        check_vma=False,
    )
```

```python
import functools
import math

import jax
import jax.numpy as jnp
from jax import lax
from jax.experimental import pallas as pl
from jax.experimental.pallas import tpu as pltpu
from jax.sharding import PartitionSpec as P

mix_rate = 0.5
CORES = 2
LANES = 128
F32 = jnp.float32
BF16 = jnp.bfloat16
SPLIT = 4
VMEM_BYTES = 67_043_328
PLACE = pltpu.VMEM
GATHERED = pltpu.VMEM


def plain_body(
    train_query, low_query, high_query, train_key, low_key, high_key, train_value, low_value, high_value,
    train_mixed, low_mixed, high_mixed, norm_train, norm_step,
):
    def merged(train, low, high):
        return (train.astype(F32) + mix_rate * jnp.dot(low, high, preferred_element_type=F32)).astype(BF16)

    return (
        lax.all_gather(merged(train_query, low_query, high_query), "zero", axis=0, tiled=True).T,
        lax.all_gather(merged(train_key, low_key, high_key), "zero", axis=0, tiled=True).T,
        lax.all_gather(merged(train_value, low_value, high_value), "zero", axis=0, tiled=True).T,
        lax.all_gather(merged(train_mixed, low_mixed, high_mixed).T, "zero", axis=0, tiled=True),
        lax.all_gather((norm_train + norm_step).astype(BF16), ("zero", "width"), axis=0, tiled=True),
    )


def kernel(
    zeros, widths,
    tq_h, lq_h, hq_h, tk_h, lk_h, hk_h, tv_h, lv_h, hv_h, tm_h, lm_h, hm_h, nt_h, ns_h,
    oq, ok, ov, om, norm_out,
    lq, hq, lk, hk, lv, hv, tm, lm, hm, nt, ns, fetched, on, own_q, own_k, own_v, own_m, pq, pk, pv, plq, plk, plv, keep, swap_send, swap_recv, send, recv, nsend, nrecv,
):
    me, w = lax.axis_index("zero"), lax.axis_index("width")
    c = lax.rem(me, 2)
    x = lax.rem(lax.div(me, 2), 2)
    y = lax.div(me, 4)
    chip = lax.div(me, 2)
    partner, xn, yn = me + 1 - 2 * c, me + 2 - 4 * x, me + 4 - 8 * y
    chip_x, chip_y, chip_d = chip + 1 - 2 * x, chip + 2 - 4 * y, 3 - chip
    rows = tq_h.shape[0]
    pair = 2 * rows

    def rank_dot(left, right):
        return lax.dot_general(left, right, (((0,), (0,)), ((), ())), preferred_element_type=F32)

    def remote(src, dst, ssem, rsem, **where):
        return pltpu.make_async_remote_copy(
            src_ref=src, dst_ref=dst, send_sem=ssem, recv_sem=rsem,
            device_id=where, device_id_type=pl.DeviceIdType.MESH,
        )

    fetches = []
    for k, (src, dst) in enumerate((
        (nt_h, nt), (ns_h, ns), (lm_h, lm), (hm_h, hm), (tm_h, tm), (tq_h, pq), (lq_h, lq.at[c]), (hq_h, hq),
        (tk_h, pk), (lk_h, lk.at[c]), (hk_h, hk), (tv_h, pv), (lv_h, lv.at[c]), (hv_h, hv),
    )):
        if k in (5, 8, 11):
            half = src.shape[1] // 2
            cols = pl.ds(pl.multiple_of(c * half, LANES), half)
            dst = dst.at[pl.ds(pl.multiple_of(rows * c, 16), rows), :]
            src = src.at[:, cols]
        copy = pltpu.make_async_copy(src, dst, fetched.at[k])
        copy.start()
        fetches.append(copy)

    others = [lax.rem(me + d, zeros) for d in range(1, zeros)]
    barrier = pltpu.get_barrier_semaphore()
    for other in others:
        pl.semaphore_signal(barrier, inc=1, device_id={"zero": other}, device_id_type=pl.DeviceIdType.MESH)
    for d in range(1, widths):
        pl.semaphore_signal(
            barrier, inc=1, device_id={"width": lax.rem(w + d, widths)}, device_id_type=pl.DeviceIdType.MESH
        )
    pl.semaphore_wait(barrier, zeros + widths - 2)

    mine = pl.ds(pl.multiple_of(rows * c, 16), rows)
    swaps = []
    for k, (train, low, held, held_low) in enumerate(((tq_h, lq_h, pq, lq), (tk_h, lk_h, pk, lk), (tv_h, lv_h, pv, lv))):
        half = train.shape[1] // 2
        cols = pl.ds(pl.multiple_of((1 - c) * half, LANES), half)
        for e, (src, dst) in enumerate(((train.at[:, cols], held.at[mine, :]), (low, held_low.at[c]))):
            copy = remote(src, dst, swap_send.at[2 * k + e], swap_recv.at[2 * k + e], zero=partner)
            copy.start()
            swaps.append(copy)

    for copy in fetches[:2]:
        copy.wait()
    on[me, w] = jnp.pad(nt[...] + ns[...], ((0, 0), (0, LANES - nt.shape[1])))
    small = []
    for d in range(1, widths):
        copy = remote(
            on.at[me, w], on.at[me, w], nsend.at[d - 1], nrecv.at[d - 1], width=lax.rem(w + d, widths)
        )
        copy.start()
        small.append(copy)

    for copy in fetches[2:5]:
        copy.wait()
    step = 2 * LANES
    for i in range(tm.shape[1] // step):
        at = slice(i * step, (i + 1) * step)
        merged = tm[:, at].astype(F32) + mix_rate * rank_dot(hm[...], lm[:, at])
        own_m[:, at] = merged.astype(BF16)
    kept = [pltpu.make_async_copy(own_m, om.at[pl.ds(pl.multiple_of(rows * me, 16), rows), :], keep.at[3])]
    kept[0].start()

    for copy in small:
        copy.wait()
    for d in range(1, zeros):
        copy = remote(
            on.at[me], on.at[me], nsend.at[widths - 2 + d], nrecv.at[widths - 2 + d], zero=others[d - 1]
        )
        copy.start()
        small.append(copy)

    part = rows // 2

    def mixed_item(h):
        return lambda p, cc: om.at[pl.ds(pl.multiple_of(rows * (2 * p + cc) + h * part, 16), part), :]

    def item(out, start, size, share):
        return lambda p, cc: out.at[
            pl.ds(pl.multiple_of(share * cc + start, 16), size), pl.ds(pl.multiple_of(pair * p, LANES), pair)
        ]

    nq, nk = oq.shape[0] // 2, ok.shape[0] // 2
    first = [mixed_item(0), item(oq, 0, nq // 2, nq), item(ok, 0, nk, nk)]
    second = [mixed_item(1), item(oq, nq // 2, nq // 2, nq), item(ov, 0, nk, nk)]
    items = first + second
    sources = [
        own_m.at[:part, :], own_q.at[: nq // 2, :], own_k, own_m.at[part:, :], own_q.at[nq // 2 :, :], own_v
    ]
    n = len(first)
    TO_X, TO_Y, ON, P_OWN, P_X, P_Y, P_D = range(7)
    copies = {}

    def go(k, kind, p, where):
        region = items[k](p, c)
        source = sources[k] if kind in (TO_X, TO_Y, P_OWN) else region
        copy = remote(source, region, send.at[k, kind], recv.at[k, kind], zero=where)
        copy.start()
        copies[k, kind] = copy

    def own(j):
        go(j, TO_X, chip, xn)
        go(n + j, TO_Y, chip, yn)

    own(0)

    def merge(e, out, own_out, held, low, held_low, high):
        half = held.shape[1]
        held_low[:, :rows] = low[0]
        held_low[:, rows:] = low[1]
        cols = pl.ds(pl.multiple_of(c * half, LANES), half)
        for j in range(pair // LANES):
            at = slice(j * LANES, (j + 1) * LANES)
            merged = held[at, :].astype(F32) + mix_rate * rank_dot(held_low[:, at], high[:, cols])
            own_out[:, at] = merged.T.astype(BF16)
        here = out.at[
            pl.ds(pl.multiple_of(c * half, 16), half), pl.ds(pl.multiple_of(pair * chip, LANES), pair)
        ]
        kept.append(pltpu.make_async_copy(own_out, here, keep.at[e]))
        kept[-1].start()

    for copy in fetches[5:] + swaps:
        copy.wait()
    merge(0, oq, own_q, pq, lq, plq, hq)
    own(1)
    merge(1, ok, own_k, pk, lk, plk, hk)
    merge(2, ov, own_v, pv, lv, plv, hv)
    own(2)
    for j in range(n):
        go(n + j, TO_X, chip, xn)
        go(j, TO_Y, chip, yn)
    for k in range(2 * n):
        go(k, P_OWN, chip, partner)

    for j in range(n):
        copies[j, TO_X].wait_recv()
        go(j, ON, chip_x, yn)
        go(j, P_X, chip_x, partner)
        copies[n + j, TO_Y].wait_recv()
        go(n + j, ON, chip_y, xn)
        go(n + j, P_Y, chip_y, partner)
    for j in range(n):
        copies[n + j, TO_X].wait_recv()
        go(n + j, P_X, chip_x, partner)
        copies[j, TO_Y].wait_recv()
        go(j, P_Y, chip_y, partner)
    for j in range(n):
        for k in (j, n + j):
            copies[k, ON].wait_recv()
            go(k, P_D, chip_d, partner)
    for copy in kept:
        copy.wait()
    for copy in small[widths - 1 :]:
        copy.wait()
    norm_out[...] = on[...]
    for (k, kind), copy in copies.items():
        copy.wait_send()
        if kind >= P_OWN:
            copy.wait_recv()


def publish(*refs):
    n = len(refs) // 2
    done = refs[-1]
    copies = []
    for k, (src, dst) in enumerate(zip(refs[:n], refs[n : 2 * n])):
        size = src.shape[0] // SPLIT
        for e in range(SPLIT):
            at = pl.ds(e * size, size)
            copies.append(pltpu.make_async_copy(src.at[at, :], dst.at[at, :], done.at[k, e]))
            copies[-1].start()
    for copy in copies:
        copy.wait()


def fast_body(zeros, widths, *args):
    tq, lq, hq, tk, lk, hk, tv, lv, hv, tm, lm, hm, nt, ns = args
    rows, depth = tq.shape[0], tq.shape[0] * zeros
    VM, HBM = pltpu.VMEM, pltpu.MemorySpace.HBM
    new = jax.ShapeDtypeStruct
    shapes = [(tq.shape[1], depth), (tk.shape[1], depth), (tv.shape[1], depth), (depth, tm.shape[0])]
    pair = 2 * rows
    held = 2 * sum(a * b for a, b in shapes)
    dma = pltpu.SemaphoreType.DMA
    small = widths - 1 + zeros - 1
    moved = [tq, lq.T, hq, tk, lk.T, hk, tv, lv.T, hv, tm.T, lm.T, hm, nt[None, :], ns[None, :]]
    local = [VM(((2,) if i in (1, 4, 7) else ()) + a.shape, a.dtype) for i, a in enumerate(moved) if i not in (0, 3, 6)]
    *full, on = pl.pallas_call(
        functools.partial(kernel, zeros, widths),
        out_shape=[GATHERED(s, BF16) for s in shapes] + [new((zeros, widths, 1, LANES), F32)],
        in_specs=[pl.BlockSpec(memory_space=HBM)] * len(args),
        out_specs=[pl.BlockSpec(memory_space=PLACE)] * len(shapes) + [pl.BlockSpec(memory_space=VM)],
        scratch_shapes=local + [
            dma((len(args),)), VM((zeros, widths, 1, LANES), F32),
            VM((tq.shape[1] // 2, pair), BF16), VM((tk.shape[1] // 2, pair), BF16), VM((tv.shape[1] // 2, pair), BF16),
            VM((tm.shape[1], tm.shape[0]), BF16),
            VM((pair, tq.shape[1] // 2), BF16), VM((pair, tk.shape[1] // 2), BF16), VM((pair, tv.shape[1] // 2), BF16),
            VM((lq.shape[1], pair), BF16), VM((lk.shape[1], pair), BF16), VM((lv.shape[1], pair), BF16),
            dma((4,)), dma((6,)), dma((6,)), dma((6, 7)), dma((6, 7)), dma((small,)), dma((small,)),
        ],
        compiler_params=pltpu.CompilerParams(
            collective_id=0, has_side_effects=True, vmem_limit_bytes=VMEM_BYTES - held - 48 * 1024
        ),
        name="gather_merged",
    )(*moved)
    norm = on[:, :, 0, : nt.shape[0]].reshape(-1).astype(BF16)
    full = pl.pallas_call(
        publish,
        out_shape=[new(s, BF16) for s in shapes],
        in_specs=[pl.BlockSpec(memory_space=PLACE)] * len(shapes),
        out_specs=[pl.BlockSpec(memory_space=HBM)] * len(shapes),
        scratch_shapes=[dma((len(shapes), SPLIT))],
        compiler_params=pltpu.CompilerParams(vmem_limit_bytes=2**20),
        name="publish",
    )(*full)
    return (*full, norm)


def solution(mesh):
    placed = (
        P("zero", "width"), P("zero", None), P(None, "width"),
        P("zero", "width"), P("zero", None), P(None, "width"),
        P("zero", "width"), P("zero", None), P(None, "width"),
        P("width", "zero"), P("width", None), P(None, "zero"),
        P(("zero", "width")), P(("zero", "width")),
    )
    zeros, widths = mesh.shape["zero"], mesh.shape["width"]
    side = math.isqrt(zeros // CORES)

    def body(*args):
        rows = args[0].shape[0]
        square = side == 2 and CORES * side * side == zeros
        if square and CORES * rows % LANES == 0 and rows % 32 == 0:
            return fast_body(zeros, widths, *args)
        return plain_body(*args)

    return jax.shard_map(
        body,
        mesh=mesh,
        in_specs=placed,
        out_specs=(P("width", None), P("width", None), P("width", None), P(None, "width"), P()),
        check_vma=False,
    )
```

```python
import functools
import math

import jax
import jax.numpy as jnp
from jax import lax
from jax.experimental import pallas as pl
from jax.experimental.pallas import tpu as pltpu
from jax.sharding import PartitionSpec as P

mix_rate = 0.5
CORES = 2
LANES = 128
F32 = jnp.float32
BF16 = jnp.bfloat16
SPLIT = 4
VMEM_BYTES = 67_043_328
PLACE = pltpu.VMEM
GATHERED = pltpu.VMEM


def plain_body(
    train_query, low_query, high_query, train_key, low_key, high_key, train_value, low_value, high_value,
    train_mixed, low_mixed, high_mixed, norm_train, norm_step,
):
    def merged(train, low, high):
        return (train.astype(F32) + mix_rate * jnp.dot(low, high, preferred_element_type=F32)).astype(BF16)

    return (
        lax.all_gather(merged(train_query, low_query, high_query), "zero", axis=0, tiled=True).T,
        lax.all_gather(merged(train_key, low_key, high_key), "zero", axis=0, tiled=True).T,
        lax.all_gather(merged(train_value, low_value, high_value), "zero", axis=0, tiled=True).T,
        lax.all_gather(merged(train_mixed, low_mixed, high_mixed).T, "zero", axis=0, tiled=True),
        lax.all_gather((norm_train + norm_step).astype(BF16), ("zero", "width"), axis=0, tiled=True),
    )


def kernel(
    zeros, widths,
    tq_h, lq_h, hq_h, tk_h, lk_h, hk_h, tv_h, lv_h, hv_h, tm_h, lm_h, hm_h, nt_h, ns_h,
    oq, ok, ov, om, norm_out,
    lq, hq, lk, hk, lv, hv, tm, lm, hm, nt, ns, fetched, on, own_q, own_k, own_v, own_m, pq, pk, pv, plq, plk, plv, keep, swap_send, swap_recv, send, recv, nsend, nrecv,
):
    me, w = lax.axis_index("zero"), lax.axis_index("width")
    c = lax.rem(me, 2)
    x = lax.rem(lax.div(me, 2), 2)
    y = lax.div(me, 4)
    chip = lax.div(me, 2)
    partner, xn, yn = me + 1 - 2 * c, me + 2 - 4 * x, me + 4 - 8 * y
    chip_x, chip_y, chip_d = chip + 1 - 2 * x, chip + 2 - 4 * y, 3 - chip
    rows = tq_h.shape[0]
    pair = 2 * rows

    def rank_dot(left, right):
        return lax.dot_general(left, right, (((0,), (0,)), ((), ())), preferred_element_type=F32)

    def remote(src, dst, ssem, rsem, **where):
        return pltpu.make_async_remote_copy(
            src_ref=src, dst_ref=dst, send_sem=ssem, recv_sem=rsem,
            device_id=where, device_id_type=pl.DeviceIdType.MESH,
        )

    fetches = []
    for k, (src, dst) in enumerate((
        (nt_h, nt), (ns_h, ns), (lm_h, lm), (hm_h, hm), (tm_h, tm), (tq_h, pq), (lq_h, lq.at[c]), (hq_h, hq),
        (tk_h, pk), (lk_h, lk.at[c]), (hk_h, hk), (tv_h, pv), (lv_h, lv.at[c]), (hv_h, hv),
    )):
        if k in (5, 8, 11):
            half = src.shape[1] // 2
            cols = pl.ds(pl.multiple_of(c * half, LANES), half)
            dst = dst.at[pl.ds(pl.multiple_of(rows * c, 16), rows), :]
            src = src.at[:, cols]
        copy = pltpu.make_async_copy(src, dst, fetched.at[k])
        copy.start()
        fetches.append(copy)

    others = [lax.rem(me + d, zeros) for d in range(1, zeros)]
    barrier = pltpu.get_barrier_semaphore()
    for other in others:
        pl.semaphore_signal(barrier, inc=1, device_id={"zero": other}, device_id_type=pl.DeviceIdType.MESH)
    for d in range(1, widths):
        pl.semaphore_signal(
            barrier, inc=1, device_id={"width": lax.rem(w + d, widths)}, device_id_type=pl.DeviceIdType.MESH
        )

    for copy in fetches[2:5]:
        copy.wait()
    step = 2 * LANES
    for i in range(tm.shape[1] // step):
        at = slice(i * step, (i + 1) * step)
        merged = tm[:, at].astype(F32) + mix_rate * rank_dot(hm[...], lm[:, at])
        own_m[:, at] = merged.astype(BF16)
    pl.semaphore_wait(barrier, zeros + widths - 2)
    kept = [pltpu.make_async_copy(own_m, om.at[pl.ds(pl.multiple_of(rows * me, 16), rows), :], keep.at[3])]
    kept[0].start()

    part = rows // 2

    def mixed_item(h):
        return lambda p, cc: om.at[pl.ds(pl.multiple_of(rows * (2 * p + cc) + h * part, 16), part), :]

    def item(out, start, size, share):
        return lambda p, cc: out.at[
            pl.ds(pl.multiple_of(share * cc + start, 16), size), pl.ds(pl.multiple_of(pair * p, LANES), pair)
        ]

    nq, nk = oq.shape[0] // 2, ok.shape[0] // 2
    last = nk // 4
    first = [mixed_item(0), item(oq, 0, nq // 2, nq), item(ok, 0, nk - last, nk), item(ok, nk - last, last, nk)]
    second = [mixed_item(1), item(oq, nq // 2, nq // 2, nq), item(ov, 0, nk - last, nk), item(ov, nk - last, last, nk)]
    items = first + second
    sources = [
        own_m.at[:part, :], own_q.at[: nq // 2, :], own_k.at[: nk - last, :], own_k.at[nk - last :, :],
        own_m.at[part:, :], own_q.at[nq // 2 :, :], own_v.at[: nk - last, :], own_v.at[nk - last :, :],
    ]
    n = len(first)
    TO_X, TO_Y, ON, P_OWN, P_X, P_Y, P_D = range(7)
    copies = {}

    def go(k, kind, p, where):
        region = items[k](p, c)
        source = sources[k] if kind in (TO_X, TO_Y, P_OWN) else region
        copy = remote(source, region, send.at[k, kind], recv.at[k, kind], zero=where)
        copy.start()
        copies[k, kind] = copy

    def own(j):
        go(j, TO_X, chip, xn)
        go(n + j, TO_Y, chip, yn)

    own(0)

    mine = pl.ds(pl.multiple_of(rows * c, 16), rows)
    swaps = []
    for k, (train, low, held, held_low) in enumerate(((tq_h, lq_h, pq, lq), (tk_h, lk_h, pk, lk), (tv_h, lv_h, pv, lv))):
        half = train.shape[1] // 2
        cols = pl.ds(pl.multiple_of((1 - c) * half, LANES), half)
        for e, (src, dst) in enumerate(((train.at[:, cols], held.at[mine, :]), (low, held_low.at[c]))):
            copy = remote(src, dst, swap_send.at[2 * k + e], swap_recv.at[2 * k + e], zero=partner)
            copy.start()
            swaps.append(copy)

    for copy in fetches[:2]:
        copy.wait()
    on[me, w] = jnp.pad(nt[...] + ns[...], ((0, 0), (0, LANES - nt.shape[1])))
    small = []
    for d in range(1, widths):
        copy = remote(
            on.at[me, w], on.at[me, w], nsend.at[d - 1], nrecv.at[d - 1], width=lax.rem(w + d, widths)
        )
        copy.start()
        small.append(copy)

    def merge(e, out, own_out, held, low, held_low, high):
        half = held.shape[1]
        held_low[:, :rows] = low[0]
        held_low[:, rows:] = low[1]
        cols = pl.ds(pl.multiple_of(c * half, LANES), half)
        for j in range(pair // LANES):
            at = slice(j * LANES, (j + 1) * LANES)
            merged = held[at, :].astype(F32) + mix_rate * rank_dot(held_low[:, at], high[:, cols])
            own_out[:, at] = merged.T.astype(BF16)
        here = out.at[
            pl.ds(pl.multiple_of(c * half, 16), half), pl.ds(pl.multiple_of(pair * chip, LANES), pair)
        ]
        kept.append(pltpu.make_async_copy(own_out, here, keep.at[e]))
        kept[-1].start()

    for copy in fetches[5:] + swaps:
        copy.wait()
    merge(0, oq, own_q, pq, lq, plq, hq)
    own(1)
    for copy in small:
        copy.wait()
    for d in range(1, zeros):
        copy = remote(
            on.at[me], on.at[me], nsend.at[widths - 2 + d], nrecv.at[widths - 2 + d], zero=others[d - 1]
        )
        copy.start()
        small.append(copy)
    merge(1, ok, own_k, pk, lk, plk, hk)
    merge(2, ov, own_v, pv, lv, plv, hv)
    own(2)
    own(3)
    for j in range(n):
        go(n + j, TO_X, chip, xn)
        go(j, TO_Y, chip, yn)
    for k in range(2 * n):
        go(k, P_OWN, chip, partner)

    for j in range(n):
        copies[j, TO_X].wait_recv()
        go(j, ON, chip_x, yn)
        go(j, P_X, chip_x, partner)
        copies[n + j, TO_Y].wait_recv()
        go(n + j, ON, chip_y, xn)
        go(n + j, P_Y, chip_y, partner)
    for j in range(n):
        copies[n + j, TO_X].wait_recv()
        go(n + j, P_X, chip_x, partner)
        copies[j, TO_Y].wait_recv()
        go(j, P_Y, chip_y, partner)
    for j in range(n):
        for k in (j, n + j):
            copies[k, ON].wait_recv()
            go(k, P_D, chip_d, partner)
    for copy in kept:
        copy.wait()
    for copy in small[widths - 1 :]:
        copy.wait()
    norm_out[...] = on[...]
    for (k, kind), copy in copies.items():
        copy.wait_send()
        if kind >= P_OWN:
            copy.wait_recv()


def publish(*refs):
    n = len(refs) // 2
    done = refs[-1]
    copies = []
    for k, (src, dst) in enumerate(zip(refs[:n], refs[n : 2 * n])):
        size = src.shape[0] // SPLIT
        for e in range(SPLIT):
            at = pl.ds(e * size, size)
            copies.append(pltpu.make_async_copy(src.at[at, :], dst.at[at, :], done.at[k, e]))
            copies[-1].start()
    for copy in copies:
        copy.wait()


def fast_body(zeros, widths, *args):
    tq, lq, hq, tk, lk, hk, tv, lv, hv, tm, lm, hm, nt, ns = args
    rows, depth = tq.shape[0], tq.shape[0] * zeros
    VM, HBM = pltpu.VMEM, pltpu.MemorySpace.HBM
    new = jax.ShapeDtypeStruct
    shapes = [(tq.shape[1], depth), (tk.shape[1], depth), (tv.shape[1], depth), (depth, tm.shape[0])]
    pair = 2 * rows
    held = 2 * sum(a * b for a, b in shapes)
    dma = pltpu.SemaphoreType.DMA
    small = widths - 1 + zeros - 1
    moved = [tq, lq.T, hq, tk, lk.T, hk, tv, lv.T, hv, tm.T, lm.T, hm, nt[None, :], ns[None, :]]
    local = [VM(((2,) if i in (1, 4, 7) else ()) + a.shape, a.dtype) for i, a in enumerate(moved) if i not in (0, 3, 6)]
    *full, on = pl.pallas_call(
        functools.partial(kernel, zeros, widths),
        out_shape=[GATHERED(s, BF16) for s in shapes] + [new((zeros, widths, 1, LANES), F32)],
        in_specs=[pl.BlockSpec(memory_space=HBM)] * len(args),
        out_specs=[pl.BlockSpec(memory_space=PLACE)] * len(shapes) + [pl.BlockSpec(memory_space=VM)],
        scratch_shapes=local + [
            dma((len(args),)), VM((zeros, widths, 1, LANES), F32),
            VM((tq.shape[1] // 2, pair), BF16), VM((tk.shape[1] // 2, pair), BF16), VM((tv.shape[1] // 2, pair), BF16),
            VM((tm.shape[1], tm.shape[0]), BF16),
            VM((pair, tq.shape[1] // 2), BF16), VM((pair, tk.shape[1] // 2), BF16), VM((pair, tv.shape[1] // 2), BF16),
            VM((lq.shape[1], pair), BF16), VM((lk.shape[1], pair), BF16), VM((lv.shape[1], pair), BF16),
            dma((4,)), dma((6,)), dma((6,)), dma((8, 7)), dma((8, 7)), dma((small,)), dma((small,)),
        ],
        compiler_params=pltpu.CompilerParams(
            collective_id=0, has_side_effects=True, vmem_limit_bytes=VMEM_BYTES - held - 48 * 1024
        ),
        name="gather_merged",
    )(*moved)
    norm = on[:, :, 0, : nt.shape[0]].reshape(-1).astype(BF16)
    full = pl.pallas_call(
        publish,
        out_shape=[new(s, BF16) for s in shapes],
        in_specs=[pl.BlockSpec(memory_space=PLACE)] * len(shapes),
        out_specs=[pl.BlockSpec(memory_space=HBM)] * len(shapes),
        scratch_shapes=[dma((len(shapes), SPLIT))],
        compiler_params=pltpu.CompilerParams(vmem_limit_bytes=2**20),
        name="publish",
    )(*full)
    return (*full, norm)


def solution(mesh):
    placed = (
        P("zero", "width"), P("zero", None), P(None, "width"),
        P("zero", "width"), P("zero", None), P(None, "width"),
        P("zero", "width"), P("zero", None), P(None, "width"),
        P("width", "zero"), P("width", None), P(None, "zero"),
        P(("zero", "width")), P(("zero", "width")),
    )
    zeros, widths = mesh.shape["zero"], mesh.shape["width"]
    side = math.isqrt(zeros // CORES)

    def body(*args):
        rows = args[0].shape[0]
        square = side == 2 and CORES * side * side == zeros
        if square and CORES * rows % LANES == 0 and rows % 32 == 0:
            return fast_body(zeros, widths, *args)
        return plain_body(*args)

    return jax.shard_map(
        body,
        mesh=mesh,
        in_specs=placed,
        out_specs=(P("width", None), P("width", None), P("width", None), P(None, "width"), P()),
        check_vma=False,
    )
```
